32 devices in a mesh: prow: 8 (over z, x), pcol: 4 (over y, core).
Axes of the slice: x: 2, y: 2, z: 4, core: 2. Of those that a mesh axis runs over, the one named last changes fastest.
Arguments:
- matrix: float32 [16384, 16384], P('prow', 'pcol'), may hold values from -6 to 6
Outputs:
- reduced: float32 [16384, 16384], P('prow', 'pcol')
- householder_coefficients: float32 [2, 8], replicated
The draws below stay inside these ranges and needn't reach their ends.
All inputs are finite; a program needn't handle non-finite values.
Results may differ from the reference program's by a relative error of at most 0.0003.
Values sent between devices are 32-bit elements; how exact they have to be, the bound alone decides.
No kernel may reach another device: no remote copies, remote signals or barrier semaphores. Data moves between devices by JAX's collectives and lax.ppermute only.
A program may use at most 128 MiB of HBM per device.

```python
import jax
import jax.numpy as jnp
from jax import lax

N = 16384
NB = 8
WINDOWS = 1


def block_scale(stream_key, shape, shards, low, high):
    loudness, own = 1.0, jax.random.fold_in(stream_key, 6)
    for dim, shards_of in shards:
        steps = jnp.exp(jax.random.uniform(jax.random.fold_in(own, dim), (shards_of,), jnp.float32, low / len(shards), high / len(shards)))
        loudness = loudness * jnp.repeat(steps, shape[dim] // shards_of).reshape([-1 if axis == dim else 1 for axis in range(len(shape))])
    return loudness


def normal_values(key, shape, spread, most, shards=(), kind=jnp.bfloat16):
    level = block_scale(key, shape, shards, -0.22, 0.18) if shards else 1.0
    values = jax.random.normal(key, shape, jnp.float32) * spread * level
    return jnp.minimum(jnp.maximum(values, -most), most).astype(kind)


def setup_inputs(seed: int = 0) -> dict:
    streams_of = jax.random.split(jax.random.key(seed), 2)
    matrix = normal_values(streams_of[0], (N, N), 1.0, 6.0, ((0, 8), (1, 4)), jnp.float32)
    return {"matrix": matrix}


epsilon = 1e-06

def precise_dot(left, right):
    return jnp.dot(left, right, precision=lax.Precision.HIGHEST)

def householder(alpha_value, sumsq):
    norm_value = jnp.sqrt(sumsq + epsilon)
    signum = jnp.where(alpha_value >= 0.0, 1.0, -1.0).astype(jnp.float32)
    beta_value = -signum * norm_value
    return (beta_value, (beta_value - alpha_value) / beta_value, alpha_value - beta_value)

def reference(matrix):
    row_index = jnp.arange(N, dtype=jnp.int32)
    col_index = jnp.arange(N, dtype=jnp.int32)
    panel_index = jnp.arange(NB, dtype=jnp.int32)
    working_array = matrix
    source_side_factor_list = []
    target_side_factor_list = []
    for window in range(WINDOWS):
        offset = window * NB
        v_rows = jnp.zeros((NB, N), jnp.float32)
        x_rows = jnp.zeros((NB, N), jnp.float32)
        y_cols = jnp.zeros((NB, N), jnp.float32)
        u_cols = jnp.zeros((NB, N), jnp.float32)
        diagonal_entries = []
        super_list = []
        for i in range(NB):
            k = offset + i
            column = working_array[:, k] - precise_dot(y_cols[:, k], v_rows) - precise_dot(u_cols[:, k], x_rows)
            masked = jnp.where(row_index >= k, column, 0.0)
            beta_left, source_side_coefficient, denom_left = householder(column[k], jnp.sum(masked * masked))
            v_new = (masked - beta_left * (row_index == k).astype(jnp.float32)) / denom_left
            transposed = precise_dot(v_new, working_array) - precise_dot(precise_dot(v_rows, v_new), y_cols) - precise_dot(precise_dot(x_rows, v_new), u_cols)
            y_new = jnp.where(col_index > k, source_side_coefficient * transposed, 0.0)
            v_rows = v_rows.at[i].set(v_new)
            y_cols = y_cols.at[i].set(y_new)
            row_eff = working_array[k, :] - precise_dot(v_rows[:, k], y_cols) - precise_dot(x_rows[:, k], u_cols)
            row_masked = jnp.where(col_index >= k + 1, row_eff, 0.0)
            right_reflector_beta, target_side_coefficient, denom_right = householder(row_eff[k + 1], jnp.sum(row_masked * row_masked))
            u_new = (row_masked - right_reflector_beta * (col_index == k + 1).astype(jnp.float32)) / denom_right
            product = precise_dot(working_array, u_new) - precise_dot(precise_dot(y_cols, u_new), v_rows) - precise_dot(precise_dot(u_cols, u_new), x_rows)
            x_new = jnp.where(row_index > k, target_side_coefficient * product, 0.0)
            x_rows = x_rows.at[i].set(x_new)
            u_cols = u_cols.at[i].set(u_new)
            diagonal_entries.append(beta_left)
            super_list.append(right_reflector_beta)
            source_side_factor_list.append(source_side_coefficient)
            target_side_factor_list.append(target_side_coefficient)
        stack_left = jnp.concatenate([v_rows, x_rows], axis=0)
        stack_right = jnp.concatenate([y_cols, u_cols], axis=0)
        updated = working_array - lax.dot_general(stack_left, stack_right, (((0,), (0,)), ((), ())), precision=lax.Precision.HIGHEST)
        updated = updated.at[offset + NB:, offset:offset + NB].set(v_rows[:, offset + NB:].T)
        row_glob = (offset + panel_index)[:, None]
        col_g = col_index[None, :]
        v_window = jnp.where(panel_index[None, :] < panel_index[:, None], v_rows[:, offset:offset + NB].T, 0.0)
        v_part = jnp.zeros((NB, N), jnp.float32).at[:, offset:offset + NB].set(v_window)
        diag_arr = jnp.stack(diagonal_entries)[:, None]
        super_arr = jnp.stack(super_list)[:, None]
        panel_values = jnp.where(col_g < offset, updated[offset:offset + NB, :], jnp.where(col_g < row_glob, v_part, jnp.where(col_g == row_glob, diag_arr, jnp.where(col_g == row_glob + 1, super_arr, u_cols))))
        working_array = updated.at[offset:offset + NB, :].set(panel_values)
    householder_coefficients = jnp.stack([jnp.stack(source_side_factor_list), jnp.stack(target_side_factor_list)])
    return (working_array, householder_coefficients)
```

```python
import jax
import jax.numpy as jnp
from jax import lax
from jax.experimental import pallas as pl
from jax.experimental.pallas import tpu as pltpu
from jax.sharding import PartitionSpec as P

NB = 8


epsilon = 1e-06


def from_root(x, axis, root):
    return lax.all_gather(x, axis)[root]


def sum_parts(long, parts, axis):
    flat = [part.reshape(-1) for part in parts]
    count = sum(part.size for part in flat)
    pad = jnp.zeros((-count % 128,), jnp.float32)
    total = jnp.sum(lax.all_gather(jnp.concatenate([long, *flat, pad]), axis), axis=0)
    outs = [total[: long.size]]
    at = long.size
    for part in parts:
        outs.append(total[at : at + part.size].reshape(part.shape))
        at += part.size
    return outs


def put_row(stack, i, row):
    at = lax.broadcasted_iota(jnp.int32, stack.shape, 0) == i
    return jnp.where(at, row[None, :], stack)


def thirds(x):
    high = lax.reduce_precision(x, 8, 7)
    rest = x - high
    middle = lax.reduce_precision(rest, 8, 7)
    low = lax.reduce_precision(rest - middle, 8, 7)
    return [part.astype(jnp.bfloat16) for part in (high, middle, low)]


def pick(n, cap):
    b = cap
    while n % b:
        b //= 2
    return b

def left_kernel(v_ref, a_ref, out_ref, acc_ref):
    step = pl.program_id(0)
    @pl.when(step == 0)
    def _():
        acc_ref[...] = jnp.zeros_like(acc_ref)
    bm, cols = a_ref.shape
    wide = jnp.concatenate([jnp.broadcast_to(v_ref[0, r:r+1, :], (128, 128)).T for r in range(bm // 128)], axis=0)
    for c in range(0, cols, 1024):
        acc = [acc_ref[:, c + 128*j: c + 128*(j+1)] for j in range(8)]
        for r in range(0, bm, 8):
            w = wide[r:r+8, :]
            for j in range(8):
                acc[j] = acc[j] + w * a_ref[r:r+8, c+128*j:c+128*(j+1)]
        for j in range(8):
            acc_ref[:, c + 128*j: c + 128*(j+1)] = acc[j]
    @pl.when(step == pl.num_programs(0) - 1)
    def _():
        out_ref[...] = jnp.sum(acc_ref[...], axis=0, keepdims=True)

def left_product(v, a, bm=256):
    rows, cols = a.shape
    bm = pick(rows, bm)
    return pl.pallas_call(
        left_kernel, grid=(rows // bm,),
        in_specs=[pl.BlockSpec((1, bm // 128, 128), lambda i: (i, 0, 0)), pl.BlockSpec((bm, cols), lambda i: (i, 0))],
        out_specs=pl.BlockSpec((1, cols), lambda i: (0, 0)),
        out_shape=jax.ShapeDtypeStruct((1, cols), jnp.float32),
        scratch_shapes=[pltpu.VMEM((8, cols), jnp.float32)],
        compiler_params=pltpu.CompilerParams(dimension_semantics=("arbitrary",), vmem_limit_bytes=48*1024*1024),
        name="left_product",
    )(v.reshape(rows // bm, bm // 128, 128), a)[0]

def right_kernel(u_ref, a_ref, out_ref):
    bm, cols = a_ref.shape
    n = cols // 128
    for g in range(bm // 128):
        part = None
        accs = [None] * 16
        for c0 in range(0, n, 16):
            us = [jnp.broadcast_to(u_ref[0:1, 128*c:128*(c+1)], (8, 128)) for c in range(c0, min(c0+16, n))]
            for q in range(16):
                r = g*128 + q*8
                acc = accs[q]
                for k, w in enumerate(us):
                    c = c0 + k
                    t = w * a_ref[r:r+8, 128*c:128*(c+1)]
                    acc = t if acc is None else acc + t
                accs[q] = acc
        full = jnp.concatenate(accs, axis=0)
        out_ref[0, g:g+1, :] = jnp.sum(full.T, axis=0, keepdims=True)

def right_product(u, a, bm=256):
    rows, cols = a.shape
    bm = pick(rows, bm)
    return pl.pallas_call(
        right_kernel, grid=(rows // bm,),
        in_specs=[pl.BlockSpec((1, cols), lambda i: (0, 0)), pl.BlockSpec((bm, cols), lambda i: (i, 0))],
        out_specs=pl.BlockSpec((1, bm // 128, 128), lambda i: (i, 0, 0)),
        out_shape=jax.ShapeDtypeStruct((rows // bm, bm // 128, 128), jnp.float32),
        compiler_params=pltpu.CompilerParams(dimension_semantics=("arbitrary",), vmem_limit_bytes=48*1024*1024),
        name="right_product",
    )(u[None], a).reshape(rows)


def precise_dot(left, right):
    return jnp.dot(left, right, precision=lax.Precision.HIGHEST)


def inner_rows(left, right):
    return lax.dot_general(left, right, (((1,), (1,)), ((), ())), precision=lax.Precision.HIGHEST)


def householder(alpha_value, sumsq):
    norm_value = jnp.sqrt(sumsq + epsilon)
    signum = jnp.where(alpha_value >= 0.0, 1.0, -1.0).astype(jnp.float32)
    beta_value = -signum * norm_value
    return (beta_value, (beta_value - alpha_value) / beta_value, alpha_value - beta_value)


def per_device(matrix):
    rows_dev, cols_dev = matrix.shape
    prow_id = lax.axis_index("prow")
    pcol_id = lax.axis_index("pcol")
    row_glob = prow_id * rows_dev + jnp.arange(rows_dev, dtype=jnp.int32)
    col_glob = pcol_id * cols_dev + jnp.arange(cols_dev, dtype=jnp.int32)
    panel_index = jnp.arange(NB, dtype=jnp.int32)
    wide_index = jnp.arange(NB + 1, dtype=jnp.int32)
    held_tile = matrix
    source_side_factor_list = []
    target_side_factor_list = []
    column_owner_rank = 0 // cols_dev
    column_local_index = 0 - column_owner_rank * cols_dev
    row_root = 0 // rows_dev
    row_local = 0 - row_root * rows_dev
    col_panel = from_root(
        held_tile[:, column_local_index : column_local_index + NB + 1].T, "pcol", column_owner_rank
    )
    half = NB // 2
    row_panel = jnp.concatenate(
        [
            from_root(held_tile[row_local + at : row_local + at + half, :], "prow", row_root)
            for at in (0, half)
        ]
    )
    sel_rows = (row_glob[None, :] == 0 + panel_index[:, None]).astype(jnp.float32)
    sel_cols = (col_glob[None, :] == 0 + wide_index[:, None]).astype(jnp.float32)
    v_rows = jnp.zeros((NB, rows_dev), jnp.float32)
    x_rows = jnp.zeros((NB, rows_dev), jnp.float32)
    y_cols = jnp.zeros((NB, cols_dev), jnp.float32)
    u_cols = jnp.zeros((NB, cols_dev), jnp.float32)
    v_panel = jnp.zeros((NB, NB), jnp.float32)
    y_panel = jnp.zeros((NB, NB + 1), jnp.float32)
    u_panel = jnp.zeros((NB, NB + 1), jnp.float32)
    diagonal_entries = []
    super_list = []
    for i in range(NB):
        column = (
            col_panel[i] - precise_dot(y_panel[:, i], v_rows) - precise_dot(u_panel[:, i], x_rows)
        )
        masked = jnp.where(row_glob >= i, column, 0.0)
        trans_part, v_coef, x_coef, col_window, col_sumsq, x_panel = sum_parts(
            left_product(masked, held_tile),
            (
                precise_dot(v_rows, masked),
                precise_dot(x_rows, masked),
                precise_dot(sel_rows, masked),
                jnp.sum(masked * masked),
                inner_rows(x_rows, sel_rows),
            ),
            "prow",
        )
        row_raw = row_panel[i]
        beta_left, source_side_coefficient, denom_left = householder(col_window[i], col_sumsq)
        row_eff = row_raw - precise_dot(v_panel[:, i], y_cols) - precise_dot(x_panel[:, i], u_cols)
        transposed = (
            trans_part
            - precise_dot(v_coef, y_cols)
            - precise_dot(x_coef, u_cols)
            - beta_left * row_eff
        ) / denom_left
        y_new = jnp.where(col_glob > i, source_side_coefficient * transposed, 0.0)
        v_new = (masked - beta_left * (row_glob == i).astype(jnp.float32)) / denom_left
        v_panel = put_row(
            v_panel,
            i,
            (col_window - beta_left * (panel_index == i).astype(jnp.float32)) / denom_left,
        )
        v_rows = put_row(v_rows, i, v_new)
        y_cols = put_row(y_cols, i, y_new)
        row_new = row_eff - y_new
        row_masked = jnp.where(col_glob >= i + 1, row_new, 0.0)
        prod_part, y_coef, u_coef, row_window, row_sumsq, y_panel = sum_parts(
            right_product(row_masked, held_tile),
            (
                precise_dot(y_cols, row_masked),
                precise_dot(u_cols, row_masked),
                precise_dot(sel_cols, row_masked),
                jnp.sum(row_masked * row_masked),
                inner_rows(y_cols, sel_cols),
            ),
            "pcol",
        )
        right_reflector_beta, target_side_coefficient, denom_right = householder(
            row_window[i + 1], row_sumsq
        )
        column_next = (
            col_panel[i + 1]
            - precise_dot(y_panel[:, i + 1], v_rows)
            - precise_dot(u_panel[:, i + 1], x_rows)
        )
        product = (
            prod_part
            - precise_dot(y_coef, v_rows)
            - precise_dot(u_coef, x_rows)
            - right_reflector_beta * column_next
        ) / denom_right
        x_new = jnp.where(row_glob > i, target_side_coefficient * product, 0.0)
        u_new = (
            row_masked - right_reflector_beta * (col_glob == i + 1).astype(jnp.float32)
        ) / denom_right
        u_panel = put_row(
            u_panel,
            i,
            (row_window - right_reflector_beta * (wide_index == i + 1).astype(jnp.float32))
            / denom_right,
        )
        x_rows = put_row(x_rows, i, x_new)
        u_cols = put_row(u_cols, i, u_new)
        diagonal_entries.append(beta_left)
        super_list.append(right_reflector_beta)
        source_side_factor_list.append(source_side_coefficient)
        target_side_factor_list.append(target_side_coefficient)
    stack_left = jnp.concatenate([v_rows, x_rows], axis=0)
    stack_right = jnp.concatenate([y_cols, u_cols], axis=0)
    lh, lm, ll = thirds(stack_left)
    rh, rm, rl = thirds(stack_right)
    updated = held_tile - lax.dot_general(
        jnp.concatenate([lh, lh, lm, lm, lh, ll], axis=0),
        jnp.concatenate([rh, rm, rh, rm, rl, rh], axis=0),
        (((0,), (0,)), ((), ())),
        preferred_element_type=jnp.float32,
    )
    col_slice = updated[:, column_local_index : column_local_index + NB]
    col_keep = jnp.logical_and(pcol_id == column_owner_rank, row_glob >= NB)[:, None]
    updated = updated.at[:, column_local_index : column_local_index + NB].set(
        jnp.where(col_keep, v_rows.T, col_slice)
    )
    row_slice = updated[row_local : row_local + NB, :]
    panel_rows_glob = (0 + panel_index)[:, None]
    col_g = col_glob[None, :]
    v_window = jnp.where(panel_index[None, :] < panel_index[:, None], v_panel.T, 0.0)
    v_part = precise_dot(v_window, sel_cols[:NB])
    diag_arr = jnp.stack(diagonal_entries)[:, None]
    super_arr = jnp.stack(super_list)[:, None]
    panel_values = jnp.where(
        col_g < 0,
        row_slice,
        jnp.where(
            col_g < panel_rows_glob,
            v_part,
            jnp.where(
                col_g == panel_rows_glob,
                diag_arr,
                jnp.where(col_g == panel_rows_glob + 1, super_arr, u_cols),
            ),
        ),
    )
    row_final = jnp.where(prow_id == row_root, panel_values, row_slice)
    held_tile = updated.at[row_local : row_local + NB, :].set(row_final)
    householder_coefficients = jnp.stack(
        [jnp.stack(source_side_factor_list), jnp.stack(target_side_factor_list)]
    )
    return (held_tile, householder_coefficients)


def solution(mesh):
    in_specs = (P("prow", "pcol"),)
    out_specs = (P("prow", "pcol"), P())
    return jax.shard_map(
        per_device, mesh=mesh, in_specs=in_specs, out_specs=out_specs, check_vma=False
    )
```
